32 devices in a mesh: row: 4 (over z), col: 8 (over y, x, core).
Axes of the slice: x: 2, y: 2, z: 4, core: 2. Of those that a mesh axis runs over, the one named last changes fastest.
Arguments:
- train_points: float32 [4, 32, 4096], P('row', None, 'col'), as said below
- targets: float32 [4, 4096], P('row', 'col'), may hold values from -16 to 16
- inverse_factor: float32 [4, 4096, 1024], P('row', 'col'), as said below
- counts: int32 [4, 4], P('row'), may hold values from 512 to 1024, as said below
- membership: int32 [4, 4, 16], replicated, may hold values from 0 to 1, as said below
- test_points: float32 [16, 32, 128], P('row'), may hold values from -6 to 6
Outputs:
- pred_mean: float32 [16, 128], P('row')
- pred_var: float32 [16, 128], P('row')
The draws below stay inside these ranges and needn't reach their ends.
Inputs may be any that keep to these rules, and one draw needn't show every extreme that they name: Each expert membership[r, c, :] takes part in at least one and at most 4 blocks, exactly 4 for at least one expert, and in at most one of the 4 blocks of each owner row. `counts`: at least one expert has all 1024 points valid. `inverse_factor`: F[i, j] as in the reference program is entry (i, j) of the inverse of the lower Cholesky factor of the expert's matrix whose entries are exp(-|x_i - x_j|^2 / 32), plus 0.1 on the diagonal, for valid i and j, and that is the identity elsewhere. `train_points`: each expert's 1024 points are drawn independently of the other experts' points.
All inputs are finite; a program needn't handle non-finite values.
Results may differ from the reference program's by a relative error of at most 0.0003.
Values sent between devices are 32-bit elements; how exact they have to be, the bound alone decides.
A program may use at most 64 MiB of HBM per device.

```python
import jax
import jax.numpy as jnp
from jax import lax

D = 32
N_PTS = 1024
BS = 128
BPR = 4
MAXB = 4
ECOL = 4
NBLK = 16
N_ROW = 4


SIGNAL = 1.0


NOISE = 0.1


def expert_points(key):
    experts_all = N_ROW * ECOL
    point_key = jax.random.fold_in(key, 11)
    points = jax.random.normal(point_key, (experts_all, N_PTS, D), jnp.float32)
    return points


def expert_counts(key):
    experts_all = N_ROW * ECOL
    drawn = jax.random.randint(jax.random.fold_in(key, 21), (experts_all,), N_PTS // 2, N_PTS + 1, jnp.int32)
    fullest = jax.random.randint(jax.random.fold_in(key, 22), (), 0, experts_all, jnp.int32)
    return drawn.at[fullest].set(N_PTS)


def factor_one(points, valid_count):
    row_valid = jnp.arange(N_PTS, dtype=jnp.int32) < valid_count
    squares = jnp.sum(points * points, axis=1)
    products = jnp.dot(points, points.T, precision=lax.Precision.HIGHEST)
    spread = squares[:, None] + squares[None, :] - 2.0 * products
    kernel = SIGNAL * jnp.exp(-spread / D)
    both_valid = row_valid[:, None] & row_valid[None, :]
    diagonal = jnp.where(row_valid, NOISE, 1.0).astype(jnp.float32)
    matrix = jnp.where(both_valid, kernel, 0.0) + jnp.diag(diagonal)
    lower = jnp.linalg.cholesky(matrix)
    identity = jnp.eye(N_PTS, dtype=jnp.float32)
    return lax.linalg.triangular_solve(lower, identity, left_side=True, lower=True)


def draw_train_points(key, part):
    experts_all = N_ROW * ECOL
    points = expert_points(key)
    stored = points.reshape(experts_all, N_PTS // 2, 2, D).transpose(0, 2, 1, 3).reshape(experts_all, N_PTS, D)
    return stored.reshape(N_ROW, ECOL, N_PTS, D).transpose(0, 3, 1, 2).reshape(N_ROW, D, ECOL * N_PTS)


def draw_inverse_factor(key, part):
    experts_all = N_ROW * ECOL
    points = expert_points(key)
    valid_counts = expert_counts(key)
    factors = lax.map(lambda expert_items: factor_one(expert_items[0], expert_items[1]), (points, valid_counts))
    stored = factors.reshape(experts_all, N_PTS // 2, 2, N_PTS).transpose(0, 2, 1, 3)
    return stored.reshape(N_ROW, ECOL * N_PTS, N_PTS)


def draw_counts(key, part):
    return expert_counts(key).reshape(N_ROW, ECOL)


def draw_membership(key, part):
    experts_all = N_ROW * ECOL
    base_key = jax.random.fold_in(key, 31)
    is_busy = jax.random.randint(jax.random.fold_in(base_key, 1), (experts_all,), 0, 8, jnp.int32) == 0
    light = jax.random.randint(jax.random.fold_in(base_key, 2), (experts_all,), 1, MAXB // 2 + 1, jnp.int32)
    taken = jnp.where(is_busy, MAXB, light).astype(jnp.int32)
    fullest = jax.random.randint(jax.random.fold_in(base_key, 3), (), 0, experts_all, jnp.int32)
    taken = taken.at[fullest].set(MAXB)
    expert_keys = jax.random.split(jax.random.fold_in(base_key, 4), experts_all)
    orders = jax.vmap(lambda one_key: jax.random.permutation(one_key, N_ROW))(expert_keys)
    places = jnp.argsort(orders, axis=1).astype(jnp.int32)
    chosen_rows = places < taken[:, None]
    block_picks = jax.random.randint(jax.random.fold_in(base_key, 5), (experts_all, N_ROW), 0, BPR, jnp.int32)
    inside = block_picks[:, :, None] == jnp.arange(BPR, dtype=jnp.int32)[None, None, :]
    member = chosen_rows[:, :, None] & inside
    return member.reshape(N_ROW, ECOL, N_ROW * BPR).astype(jnp.int32)


def block_scale(stream_key, dims, cuts, least, top_value):
    def one(axis_at, parts):
        heights = jax.random.uniform(jax.random.fold_in(jax.random.fold_in(stream_key, 6), axis_at), (parts,), jnp.float32, least / len(cuts), top_value / len(cuts))
        return jnp.repeat(jnp.exp(heights), dims[axis_at] // parts).reshape((-1,) + (1,) * (len(dims) - axis_at - 1))

    loudness = one(*cuts[0])
    for cut in cuts[1:]:
        loudness = loudness * one(*cut)
    return loudness


def bell_draw(rng, dims, deviation, limit, shards=(), kind=jnp.bfloat16):
    gain = block_scale(rng, dims, shards, -0.22, 0.18) if shards else 1.0
    values = jax.random.normal(rng, dims, jnp.float32) * deviation * gain
    return jnp.minimum(jnp.maximum(values, -limit), limit).astype(kind)


def setup_inputs(seed: int = 0) -> dict:
    streams_of = jax.random.split(jax.random.key(seed), 7)
    return {
        "train_points": draw_train_points(jax.random.fold_in(streams_of[6], 71), 0),
        "targets": bell_draw(streams_of[1], (N_ROW, ECOL * N_PTS), 3.0, 16.0, ((0, 4), (1, 8)), jnp.float32),
        "inverse_factor": draw_inverse_factor(jax.random.fold_in(streams_of[6], 71), 0),
        "counts": draw_counts(jax.random.fold_in(streams_of[6], 71), 0),
        "membership": draw_membership(jax.random.fold_in(streams_of[6], 71), 0),
        "test_points": bell_draw(streams_of[5], (NBLK, D, BS), 1.0, 6.0, ((0, 4),), jnp.float32),
    }


SIGNAL = 1.0
NOISE = 0.1
HIGHEST = lax.Precision.HIGHEST

def cross_kernel(train_cols, test_cols, squared_scale):
    products = jnp.einsum('dn,dp->np', train_cols, test_cols, precision=HIGHEST)
    spread = jnp.sum(train_cols * train_cols, axis=0)[:, None] + jnp.sum(test_cols * test_cols, axis=0)[None, :] - 2.0 * products
    return SIGNAL * jnp.exp(-0.5 * spread / squared_scale)

def slot_table(member, slot_count):
    member_flags = member.astype(jnp.int32)
    before = jnp.cumsum(member_flags) - member_flags
    slot_ids = jnp.arange(slot_count, dtype=jnp.int32)[:, None]
    picked = ((member_flags[None, :] == 1) & (before[None, :] == slot_ids)).astype(jnp.int32)
    chosen = jnp.sum(picked * jnp.arange(member.shape[0], dtype=jnp.int32)[None, :], axis=1).astype(jnp.int32)
    return (picked.astype(jnp.float32), chosen)

def weigh_expert(mean_part, quad_part):
    variance = NOISE + jnp.maximum(SIGNAL - quad_part, 0.0)
    entropy_gap = 0.5 * (jnp.log(SIGNAL + NOISE) - jnp.log(variance))
    weight = entropy_gap / variance
    return (weight * mean_part, weight)

def reference(train_points, targets, inverse_factor, counts, membership, test_points):
    features = train_points.shape[1]
    squared_scale = 0.5 * features
    experts_all = N_ROW * ECOL
    half_pts = N_PTS // 2
    train_all = train_points.reshape(N_ROW, features, ECOL, N_PTS).transpose(0, 2, 1, 3).reshape(experts_all, features, 2, half_pts)
    train_all = train_all.transpose(0, 1, 3, 2).reshape(experts_all, features, N_PTS)
    target_all = targets.reshape(experts_all, 2, half_pts).transpose(0, 2, 1).reshape(experts_all, N_PTS)
    factor_all = inverse_factor.reshape(experts_all, 2, half_pts, N_PTS).transpose(0, 2, 1, 3).reshape(experts_all, N_PTS, N_PTS)
    count_all = counts.reshape(experts_all)
    member_all = membership.reshape(experts_all, NBLK)

    def accumulate(totals, expert_items):
        train_cols, target_col, factor, valid_count, member = expert_items
        picked, chosen = slot_table(member, MAXB)
        test_cols = test_points[chosen].transpose(1, 0, 2).reshape(features, MAXB * BS)
        row_valid = jnp.arange(N_PTS, dtype=jnp.int32) < valid_count
        kernel = jnp.where(row_valid[:, None], cross_kernel(train_cols, test_cols, squared_scale), 0.0)
        solved = jnp.dot(factor.astype(jnp.float32), kernel.astype(jnp.float32), precision=HIGHEST, preferred_element_type=jnp.float32)
        whitened = jnp.dot(factor.astype(jnp.float32), target_col.astype(jnp.float32), precision=HIGHEST, preferred_element_type=jnp.float32)
        mean_part = jnp.dot(whitened.astype(jnp.float32), solved.astype(jnp.float32), precision=HIGHEST, preferred_element_type=jnp.float32)
        quad_part = jnp.sum(solved * solved, axis=0)
        weighted, weight = weigh_expert(mean_part, quad_part)
        dense_num = jnp.einsum('sb,sp->bp', picked, weighted.reshape(MAXB, BS), precision=HIGHEST)
        dense_wgt = jnp.einsum('sb,sp->bp', picked, weight.reshape(MAXB, BS), precision=HIGHEST)
        return ((totals[0] + dense_num, totals[1] + dense_wgt), None)
    start = (jnp.zeros((NBLK, BS), jnp.float32), jnp.zeros((NBLK, BS), jnp.float32))
    totals, _ = lax.scan(accumulate, start, (train_all, target_all, factor_all, count_all, member_all))
    precision_sum = 1.0 / (SIGNAL + NOISE) + totals[1]
    return (totals[0] / precision_sum, 1.0 / precision_sum)
```

```python
import functools
import math

import jax
import jax.numpy as jnp
from jax import lax
from jax.experimental import pallas as pl
from jax.experimental.pallas import tpu as pltpu
from jax.sharding import PartitionSpec as P

SIGNAL = 1.0
NOISE = 0.1
F32 = jnp.float32
BF16 = jnp.bfloat16
MESH = pl.DeviceIdType.MESH
LANES = 128
FAR = 2.0 ** 15


def high_low(value):
    high = value.astype(BF16)
    return high, (value - high.astype(F32)).astype(BF16)


def three_parts(value):
    a = value.astype(BF16).astype(F32)
    b = (value - a).astype(BF16).astype(F32)
    return a, b, value - a - b


def in_rows(parts, width):
    at = lax.broadcasted_iota(jnp.int32, (8, width), 0)
    tail = jnp.zeros((8, width), F32)
    for i, v in parts:
        tail = jnp.where(at == i, v, tail)
    return tail


def folded(value):
    rows, width = value.shape
    return jnp.sum(value.reshape(rows // 8, 8, width), axis=0)


def expert_kernel(
    rows, cols,
    counts_hbm, member_hbm, train_ref, target_ref, factor_ref, test_ref,
    sums_ref,
    factor_buf, own_x, own_y, tests, other_x, other_y, sent_tests, got_tests,
    stack, nat_a, nat_b, points, k_cat, white,
    sent_parts, got_parts, taken_by, sent_bytes, counts_ref, member_ref,
    local_sems, factor_sems, x_send, x_recv, t_send, t_recv, p_send, p_recv,
):
    row = lax.axis_index("row")
    col = lax.axis_index("col")
    parity = col % 2
    expert = col // 2
    experts = cols // 2
    blocks, features, length = tests.shape
    half = own_x.shape[1]
    tall = 2 * LANES
    steps = half // LANES
    partner = (row, expert * 2 + 1 - parity)

    others = [lax.rem(row + d, rows) for d in range(1, rows)]
    mates = [lax.rem(expert + d, experts) for d in range(1, experts)]
    barrier = pltpu.get_barrier_semaphore()
    peers = [partner]
    for r in others:
        peers += [(r, expert * 2), (r, expert * 2 + 1)]
    for c in mates:
        peers += [(row, c * 2), (row, c * 2 + 1)]
    for peer in peers:
        pl.semaphore_signal(barrier, inc=1, device_id=peer, device_id_type=MESH)

    load_member = pltpu.make_async_copy(member_hbm, member_ref, local_sems.at[4])
    load_counts = pltpu.make_async_copy(counts_hbm, counts_ref, local_sems.at[5])
    load_tests = pltpu.make_async_copy(test_ref, tests, local_sems.at[0])
    load_x = pltpu.make_async_copy(train_ref.at[0], own_x, local_sems.at[1])
    load_y = pltpu.make_async_copy(target_ref, own_y, local_sems.at[2])
    load_member.start()
    load_tests.start()
    load_x.start()
    load_y.start()
    load_counts.start()
    loads = []
    for b in range(steps):
        part = (pl.ds(b * LANES, LANES), pl.ds(0, tall * (b + 1)))
        loads.append(pltpu.make_async_copy(
            factor_ref.at[0].at[part], factor_buf.at[part], factor_sems.at[b]))
        loads[b].start()

    def chosen_in(row_at, owner):
        at = jnp.int32(0)
        for j in range(1, blocks):
            at = at + j * member_ref[row_at, expert, owner * blocks + j]
        return at

    load_member.wait()
    load_tests.wait()
    for d, r in enumerate(others):
        sent_tests[d] = tests[chosen_in(r, row)]
    load_x.wait()
    load_y.wait()
    pl.semaphore_wait(barrier, len(peers))

    def remote(src, dst, send, recv, peer):
        copy = pltpu.make_async_remote_copy(
            src_ref=src, dst_ref=dst, send_sem=send, recv_sem=recv,
            device_id=peer, device_id_type=MESH,
        )
        copy.start()
        return copy

    test_copies = [
        remote(sent_tests.at[d], got_tests.at[d], t_send.at[d], t_recv.at[d],
               (r, col))
        for d, r in enumerate(others)
    ]
    x_copy = remote(own_x, other_x, x_send.at[0], x_recv.at[0], partner)
    y_copy = remote(own_y, other_y, x_send.at[1], x_recv.at[1], partner)

    load_counts.wait()
    valid = counts_ref[0, expert]
    scale = math.log2(math.e) / features

    def stacked(x, y, offset):
        at = 2 * lax.broadcasted_iota(jnp.int32, (1, half), 1) + offset
        inside = at < valid
        x = jnp.where(inside, x, 0.0)
        xh = x.astype(BF16).astype(F32)
        xl = x - xh
        a, b, c = three_parts(scale * jnp.sum(x * x, axis=0, keepdims=True))
        a = jnp.where(inside, a, FAR)
        yh = y.astype(BF16).astype(F32)
        one = jnp.ones((1, half), F32)
        tail = in_rows(
            enumerate((a, b, c, yh, y - yh, one, one, one)), half)
        first = jnp.concatenate([xh, xl, xh, xl], axis=0)
        last = jnp.concatenate([tail, jnp.zeros((LANES - 8, half), F32)], axis=0)
        return first.T, last.T

    def put(a, b, offset):
        nat_a[pl.ds(offset, half, stride=2), :] = a
        nat_b[pl.ds(offset, half, stride=2), :] = b

    a, b = stacked(own_x[...], own_y[...], parity)

    @pl.when(parity == 0)
    def _():
        put(a, b, 0)

    @pl.when(parity == 1)
    def _():
        put(a, b, 1)

    for b in range(steps):
        loads[b].wait()
        width = tall * (b + 1)
        fh, fl = high_low(factor_buf[b * LANES:(b + 1) * LANES, :width])
        stack[b * tall:b * tall + LANES, :width] = fh
        stack[b * tall + LANES:(b + 1) * tall, :width] = fl

    x_copy.wait_recv()
    y_copy.wait_recv()
    a2, b2 = stacked(other_x[...], other_y[...], 1 - parity)

    @pl.when(parity == 1)
    def _():
        put(a2, b2, 0)

    @pl.when(parity == 0)
    def _():
        put(a2, b2, 1)

    points[:, :LANES] = nat_a[...].astype(BF16)
    points[:, LANES:] = nat_b[...].astype(BF16)
    for b in range(steps):
        width = tall * (b + 1)
        out = jnp.dot(stack[b * tall:(b + 1) * tall, :width],
                      points[:width, LANES:], preferred_element_type=F32)
        both = out[:LANES] + out[LANES:]
        line = both[:, 3:4] + both[:, 4:5]
        white[b * LANES:(b + 1) * LANES, :] = jnp.broadcast_to(line, (LANES, length))

    order = [None] + list(range(rows - 1))
    owners = [row] + [lax.rem(row + rows - d - 1, rows) for d in range(rows - 1)]
    for s in range(rows):
        d = order[s]
        if d is None:
            t = tests[chosen_in(row, row)]
        else:
            test_copies[d].wait_recv()
            t = got_tests[d]
        th, tl = high_low((2.0 * scale) * t)
        t2 = three_parts(-scale * jnp.sum(t * t, axis=0, keepdims=True))
        minus = jnp.full((1, length), -1.0, F32)
        tail = in_rows([*enumerate((minus,) * 3), *enumerate(t2, 5)], length)
        last = jnp.concatenate(
            [tail, jnp.zeros((LANES - 8, length), F32)], axis=0).astype(BF16)
        rhs = jnp.concatenate([th, th, tl, tl, last], axis=0)
        mean = jnp.zeros((8, length), F32)
        quad = jnp.zeros((8, length), F32)
        for b in range(steps):
            at = slice(b * tall, (b + 1) * tall)
            k = SIGNAL * jnp.exp2(
                jnp.dot(points[at, :], rhs, preferred_element_type=F32))
            kh, kl = high_low(k)
            k_cat[at, :length] = kh
            k_cat[at, length:] = kl
        for b in range(steps):
            at = slice(b * tall, (b + 1) * tall)
            out = jnp.dot(stack[at, :tall * (b + 1)], k_cat[:tall * (b + 1), :],
                          preferred_element_type=F32)
            both = out[:LANES] + out[LANES:]
            solved = both[:, :length] + both[:, length:]
            quad += folded(solved * solved)
            mean += folded(solved * white[b * LANES:(b + 1) * LANES, :])
        sent_parts[s, 0:1, :] = jnp.sum(mean, axis=0, keepdims=True)
        sent_parts[s, 1:2, :] = jnp.sum(quad, axis=0, keepdims=True)
        mine = got_parts.at[expert, parity, row]
        if d is None:
            keep = pltpu.make_async_copy(sent_parts.at[s], mine, p_recv.at[0])
            keep.start()
            targets = [partner]
            for c in mates:
                targets += [(row, c * 2), (row, c * 2 + 1)]
        else:
            targets = [(owners[s], lax.rem(col + c, cols)) for c in range(cols)]
        for target in targets:
            remote(sent_parts.at[s], mine, p_send.at[s], p_recv.at[0], target)

    for j in range(blocks):
        for e in range(experts):
            for r in range(rows):
                on = member_ref[r, e, row * blocks + j]
                n = e * rows + r
                taken_by[j, n:n + 1, :] = jnp.full((1, length), on, jnp.int32).astype(F32)

    pltpu.make_async_copy(got_parts, got_parts, p_recv.at[0]).wait()
    total = got_parts[:, 0] + got_parts[:, 1]
    total = total.reshape(experts * rows, 2, length)
    mean = total[:, 0, :]
    quad = total[:, 1, :]
    variance = NOISE + jnp.maximum(SIGNAL - quad, 0.0)
    gap = 0.5 * (jnp.log(jnp.full_like(variance, SIGNAL + NOISE)) - jnp.log(variance))
    weight = gap / variance
    weighted = weight * mean
    for j in range(blocks):
        on = taken_by[j] > 0.5
        sums_ref[j:j + 1, :] = jnp.sum(jnp.where(on, weighted, 0.0), axis=0, keepdims=True)
        sums_ref[blocks + j:blocks + j + 1, :] = jnp.sum(
            jnp.where(on, weight, 0.0), axis=0, keepdims=True)
    x_copy.wait_send()
    y_copy.wait_send()
    for copy in test_copies:
        copy.wait_send()
    for s in range(rows):
        sent = cols - 1 if order[s] is None else cols
        flat = sent_bytes.at[pl.ds(0, sent)]
        pltpu.make_async_copy(flat, flat, p_send.at[s]).wait()


def on_device(rows, cols, train_points, targets, inverse_factor, counts, membership, test_points):
    features, half = train_points.shape[1:]
    blocks, _, length = test_points.shape
    points = inverse_factor.shape[2]
    experts = cols // 2
    vmem, dma = pltpu.VMEM, pltpu.SemaphoreType.DMA
    anywhere = pl.BlockSpec(memory_space=pltpu.HBM)
    sums = pl.pallas_call(
        functools.partial(expert_kernel, rows, cols),
        out_shape=pltpu.VMEM((2 * blocks, length), F32),
        in_specs=[anywhere] * 6,
        out_specs=pl.BlockSpec(memory_space=pltpu.VMEM),
        scratch_shapes=[
            vmem((half, points), F32),
            vmem((features, half), F32),
            vmem((1, half), F32),
            vmem((blocks, features, length), F32),
            vmem((features, half), F32),
            vmem((1, half), F32),
            vmem((rows - 1, features, length), F32),
            vmem((rows - 1, features, length), F32),
            vmem((2 * half, points), BF16),
            vmem((points, LANES), F32),
            vmem((points, LANES), F32),
            vmem((points, 2 * LANES), BF16),
            vmem((points, 2 * length), BF16),
            vmem((half, length), F32),
            vmem((rows, 2, length), F32),
            vmem((experts, 2, rows, 2, length), F32),
            vmem((blocks, experts * rows, length), F32),
            vmem((cols, 2, length), F32),
            pltpu.SMEM(counts.shape, jnp.int32),
            pltpu.SMEM(membership.shape, jnp.int32),
            dma((6,)),
            dma((half // LANES,)),
            dma((2,)),
            dma((2,)),
            dma((rows - 1,)),
            dma((rows - 1,)),
            dma((rows,)),
            dma((1,)),
        ],
        compiler_params=pltpu.CompilerParams(
            collective_id=0, has_side_effects=True
        ),
    )(counts, membership, train_points, targets, inverse_factor, test_points)
    precision_sum = 1.0 / (SIGNAL + NOISE) + sums[blocks:]
    return (sums[:blocks] / precision_sum, 1.0 / precision_sum)


def solution(mesh):
    in_specs = (
        P("row", None, "col"),
        P("row", "col"),
        P("row", "col", None),
        P("row", None),
        P(),
        P("row", None, None),
    )
    out_specs = (P("row", None), P("row", None))
    body = functools.partial(on_device, mesh.shape["row"], mesh.shape["col"])
    return jax.shard_map(
        body, mesh=mesh, in_specs=in_specs, out_specs=out_specs, check_vma=False
    )
```
